32 devices in a mesh: sweep: 4 (over z), layer: 8 (over y, x, core).
Axes of the slice: x: 2, y: 2, z: 4, core: 2. Of those that a mesh axis runs over, the one named last changes fastest.
Arguments:
- green: bfloat16 [4, 2, 8192, 8192], P('sweep', None, 'layer'), may hold values from -1 to 1
- down_source: float32 [4, 2, 16, 8192], P('sweep', None, None, 'layer'), may hold values from -6 to 6
- up_source: float32 [4, 2, 16, 8192], P('sweep', None, None, 'layer'), may hold values from -6 to 6
Outputs:
- total: float32 [4, 2, 16, 8192], P('sweep', None, None, 'layer')
The draws below stay inside these ranges and needn't reach their ends.
All inputs are finite; a program needn't handle non-finite values.
Results may differ from the reference program's by a relative error of at most 0.02.
Values may be sent and summed in bfloat16 or wider, within the bound.
A program may use at most 64 MiB of HBM per device.

```python
import math
import jax
import jax.numpy as jnp
from jax import lax

W = 8192
SOURCES = 16
LAYERS = 4


def draw_green(key, part):
    base_key = jax.random.fold_in(key, 7)
    spread = 0.5 / math.sqrt(2.0 * W)

    def draw_layer(layer_index):
        layer_key = jax.random.fold_in(base_key, layer_index)
        key_offdiag, key_modulus, key_angles = jax.random.split(layer_key, 3)
        offdiag = jax.random.normal(key_offdiag, (2, W, W), jnp.float32) * spread
        modulus = jax.random.uniform(key_modulus, (W,), jnp.float32, 0.6, 0.9)
        angles = jax.random.uniform(key_angles, (W,), jnp.float32, -jnp.pi, jnp.pi)
        diagonal = jnp.stack([modulus * jnp.cos(angles), modulus * jnp.sin(angles)])
        row_ids = lax.broadcasted_iota(jnp.int32, (W, W), 0)
        col_ids = lax.broadcasted_iota(jnp.int32, (W, W), 1)
        on_diagonal = jnp.where(row_ids == col_ids, 1.0, 0.0).astype(jnp.float32)
        matrix = offdiag + on_diagonal[None] * diagonal[:, :, None]
        matrix = jnp.clip(matrix, -1.0, 1.0)
        return matrix.astype(jnp.bfloat16)
    return lax.map(draw_layer, jnp.arange(LAYERS, dtype=jnp.int32))


def steps_of(own_key, shape, cuts, least, high):
    level, own = 1.0, jax.random.fold_in(own_key, 6)
    for axis_at, shards_of in cuts:
        heights = jnp.exp(jax.random.uniform(jax.random.fold_in(own, axis_at), (shards_of,), jnp.float32, least / len(cuts), high / len(cuts)))
        level = level * jnp.repeat(heights, shape[axis_at] // shards_of).reshape([-1 if axis == axis_at else 1 for axis in range(len(shape))])
    return level


def bell_draw(stream_key, shape, deviation, reach, cuts=(), held_as=jnp.bfloat16):
    factor_of = steps_of(stream_key, shape, cuts, -0.22, 0.18) if cuts else 1.0
    array = jax.random.normal(stream_key, shape, jnp.float32) * deviation * factor_of
    return jnp.minimum(jnp.maximum(array, -reach), reach).astype(held_as)


def setup_inputs(seed: int = 0) -> dict:
    streams_of = jax.random.split(jax.random.key(seed), 4)
    green = draw_green(jax.random.fold_in(streams_of[3], 71), 0)
    down_source = bell_draw(streams_of[1], (LAYERS, 2, SOURCES, W), 1.0, 6.0, ((0, 4), (3, 8)), jnp.float32)
    up_source = bell_draw(streams_of[2], (LAYERS, 2, SOURCES, W), 1.0, 6.0, ((0, 4), (3, 8)), jnp.float32)
    return {"green": green, "down_source": down_source, "up_source": up_source}


def rows_product(trace_in, matrix):
    contract = (((1,), (1,)), ((), ()))
    real_real = lax.dot_general(trace_in[0], matrix[0], contract, preferred_element_type=jnp.float32)
    imag_imag = lax.dot_general(trace_in[1], matrix[1], contract, preferred_element_type=jnp.float32)
    real_imag = lax.dot_general(trace_in[0], matrix[1], contract, preferred_element_type=jnp.float32)
    imag_real = lax.dot_general(trace_in[1], matrix[0], contract, preferred_element_type=jnp.float32)
    return jnp.stack([real_real - imag_imag, real_imag + imag_real])


def cols_product(trace_in, matrix):
    real_real = jnp.dot(trace_in[0], matrix[0], preferred_element_type=jnp.float32)
    imag_imag = jnp.dot(trace_in[1], matrix[1], preferred_element_type=jnp.float32)
    real_imag = jnp.dot(trace_in[0], matrix[1], preferred_element_type=jnp.float32)
    imag_real = jnp.dot(trace_in[1], matrix[0], preferred_element_type=jnp.float32)
    return jnp.stack([real_real - imag_imag, real_imag + imag_real])


def reference(green, down_source, up_source):
    layers = green.shape[0]
    outgoing = jnp.zeros((2, SOURCES, W), jnp.bfloat16)
    down_list = []
    for layer_index in range(layers):
        down_row = down_source[layer_index] + rows_product(outgoing, green[layer_index])
        down_list.append(down_row)
        outgoing = down_row.astype(jnp.bfloat16)
    outgoing = jnp.zeros((2, SOURCES, W), jnp.bfloat16)
    total_list = [None] * layers
    for layer_index in reversed(range(layers)):
        total_row = (up_source[layer_index] + down_list[layer_index]) + cols_product(outgoing, green[layer_index])
        total_list[layer_index] = total_row
        outgoing = total_row.astype(jnp.bfloat16)
    return jnp.stack(total_list)
```

```python
import functools

import jax
import jax.numpy as jnp
from jax import lax
from jax.experimental import pallas as pl
from jax.experimental.pallas import tpu as pltpu
from jax.sharding import PartitionSpec as P

MESH = pl.DeviceIdType.MESH
F32, BF16 = jnp.float32, jnp.bfloat16
BY_LANES = (((1,), (1,)), ((), ()))


def turned(trace):
    half = trace.shape[0] // 2
    return jnp.concatenate([-trace[half:], trace[:half]], axis=0)


def rows_dot(trace, block):
    return lax.dot_general(trace, block, BY_LANES, preferred_element_type=F32)


def cols_dot(trace, block):
    return jnp.dot(trace, block, preferred_element_type=F32)


def sweeps(layers, peers, blocks, green, down_src, up_src, total,
           matrix, gathered, incoming, part_out, part_in, out_down, out_up, base, acc,
           load_sem, dsend, drecv, gsend, grecv, usend, urecv, psend, precv):
    z, j = lax.axis_index("sweep"), lax.axis_index("layer")
    own = down_src.shape[1]
    width = own // blocks
    odd = lax.rem(z, 2) == 1

    def span(k):
        return pl.ds(pl.multiple_of(k * width, width), width)

    def cols(i, k):
        return pl.ds(pl.multiple_of(i * own + k * width, width), width)

    def peer(d):
        return lax.rem(j + d, peers)

    def load(m, part):
        return pltpu.make_async_copy(
            green.at[part, span(m)], matrix.at[part, span(m)], load_sem.at[m, part])

    def wait_load(m):
        load(m, 0).wait()
        load(m, 1).wait()

    def remote(src, dst, send, recv, to):
        return pltpu.make_async_remote_copy(
            src_ref=src, dst_ref=dst, send_sem=send, recv_sem=recv, device_id=to, device_id_type=MESH)

    def pass_down(k):
        return remote(out_down.at[k], gathered.at[k, j], dsend.at[k], drecv.at[k], {"sweep": z + 1})

    def pass_up(k):
        return remote(out_up.at[k], incoming.at[k], usend.at[k], urecv.at[k], {"sweep": z - 1})

    def relay(k, d):
        return remote(gathered.at[k, j], gathered.at[k, j], gsend.at[k, d], grecv.at[k, j], {"layer": peer(d)})

    def relayed(k, d):
        i = peer(d)
        return remote(gathered.at[k, i], gathered.at[k, i], gsend.at[k, d], grecv.at[k, i], {"layer": i})

    def share(d, k):
        i = peer(d)
        return remote(part_out.at[i, k], part_in.at[j, k], psend.at[d, k], precv.at[j, k], {"layer": i})

    def shared(d, k):
        i = peer(d)
        return remote(part_out.at[i, k], part_in.at[i, k], psend.at[d, k], precv.at[i, k], {"layer": i})

    def share_all(d):
        i = peer(d)
        return remote(part_out.at[i], part_in.at[j], psend.at[d, 0], precv.at[j, 0], {"layer": i})

    def shared_all(d):
        i = peer(d)
        return remote(part_out.at[i], part_in.at[i], psend.at[d, 0], precv.at[i, 0], {"layer": i})

    for m in range(blocks):
        load(m, 0).start()
        load(m, 1).start()

    barrier = pltpu.get_barrier_semaphore()
    for d in range(1, peers):
        pl.semaphore_signal(barrier, inc=1, device_id={"layer": peer(d)}, device_id_type=MESH)
    for step in (1, layers - 1):
        pl.semaphore_signal(barrier, inc=1, device_id={"sweep": lax.rem(z + step, layers)}, device_id_type=MESH)
    pl.semaphore_wait(barrier, peers + 1)

    def finish_down(k, value):
        sum_of = up_src[:, span(k)] + value

        @pl.when(z < layers - 1)
        def _():
            base[:, span(k)] = sum_of
            out_down[k] = value.astype(BF16)
            pass_down(k).start()

        @pl.when(z == layers - 1)
        def _():
            total[:, span(k)] = sum_of
            out_up[k] = sum_of.astype(BF16)
            pass_up(k).start()

    def take(k):
        relayed_own = remote(
            out_down.at[k], gathered.at[k, j], dsend.at[k], drecv.at[k], {"sweep": z})
        relayed_own.wait_recv()
        for d in range(1, peers):
            relay(k, d).start()

    def wait_gather(k):
        for d in range(1, peers):
            relayed(k, d).wait_recv()

    def wait_up(k):
        remote(out_up.at[k], incoming.at[k], usend.at[k], urecv.at[k], {"sweep": z}).wait_recv()

    @pl.when(z == 0)
    def _():
        @pl.loop(0, blocks)
        def _(k):
            finish_down(k, down_src[:, span(k)])

        @pl.loop(0, blocks)
        def _(m):
            wait_load(m)

    @pl.when(odd)
    def _():
        @pl.loop(0, blocks)
        def _(k):
            take(k)

        @pl.loop(0, blocks)
        def _(k):
            wait_gather(k)

        @pl.loop(0, blocks)
        def _(m):
            wait_load(m)
            value = None
            for k in range(blocks):
                for i in range(peers):
                    trace = gathered[k, i]
                    term = rows_dot(trace, matrix[0, span(m), cols(i, k)])
                    value = term if value is None else value + term
                    value = value + rows_dot(turned(trace), matrix[1, span(m), cols(i, k)])
            finish_down(m, down_src[:, span(m)] + value)

    @pl.when(jnp.logical_not(odd) & (z > 0))
    def _():
        @pl.loop(0, blocks)
        def _(m):
            wait_load(m)

        base[...] = down_src[...]
        take(0)

        @pl.loop(0, blocks)
        def _(k):
            @pl.when(k + 1 < blocks)
            def _():
                take(k + 1)

            wait_gather(k)
            for m in range(blocks):
                value = None
                for i in range(peers):
                    trace = gathered[k, i]
                    term = rows_dot(trace, matrix[0, span(m), cols(i, k)])
                    value = term if value is None else value + term
                    value = value + rows_dot(turned(trace), matrix[1, span(m), cols(i, k)])
                base[:, span(m)] += value

        @pl.loop(0, blocks)
        def _(k):
            finish_down(k, base[:, span(k)])

    def finish_up(k):
        value = acc[j, :, span(k)]
        for d in range(1, peers):
            value = value + part_in[peer(d), k].astype(F32)
        value = base[:, span(k)] + value
        total[:, span(k)] = value

        @pl.when(z > 0)
        def _():
            out_up[k] = value.astype(BF16)
            pass_up(k).start()

    @pl.when(odd & (z < layers - 1))
    def _():
        @pl.loop(0, blocks)
        def _(k):
            wait_up(k)

        def reduce(k):
            for d in range(1, peers):
                shared(d, k).wait_recv()
            finish_up(k)

        @pl.loop(0, blocks)
        def _(k):
            for d in list(range(1, peers)) + [0]:
                i = peer(d)
                value = None
                for r in range(blocks):
                    trace = incoming[r]
                    term = cols_dot(trace, matrix[0, span(r), cols(i, k)])
                    value = term if value is None else value + term
                    value = value + cols_dot(turned(trace), matrix[1, span(r), cols(i, k)])
                if d:
                    part_out[i, k] = value.astype(BF16)
                else:
                    acc[i, :, span(k)] = value
            for d in range(1, peers):
                share(d, k).start()

            @pl.when(k > 0)
            def _():
                reduce(k - 1)

        reduce(blocks - 1)

        @pl.loop(0, blocks)
        def _(k):
            for d in range(1, peers):
                share(d, k).wait_send()

    @pl.when(jnp.logical_not(odd) & (z < layers - 1))
    def _():
        acc[...] = jnp.zeros_like(acc)

        @pl.loop(0, blocks)
        def _(r):
            wait_up(r)
            trace = incoming[r]
            for i in range(peers):
                for k in range(blocks):
                    value = cols_dot(trace, matrix[0, span(r), cols(i, k)])
                    value = value + cols_dot(turned(trace), matrix[1, span(r), cols(i, k)])
                    acc[i, :, span(k)] += value

        for d in range(1, peers):
            i = peer(d)
            for k in range(blocks):
                part_out[i, k] = acc[i, :, span(k)].astype(BF16)
            share_all(d).start()
        for d in range(1, peers):
            shared_all(d).wait_recv()

        @pl.loop(0, blocks)
        def _(k):
            finish_up(k)

        for d in range(1, peers):
            share_all(d).wait_send()

    @pl.when(z < layers - 1)
    def _():
        @pl.loop(0, blocks)
        def _(k):
            pass_down(k).wait_send()

    @pl.when(z > 0)
    def _():
        @pl.loop(0, blocks)
        def _(k):
            pass_up(k).wait_send()
            for d in range(1, peers):
                relay(k, d).wait_send()


def local(layers, peers, green, down_source, up_source):
    _one, parts, own, wide = green.shape
    sources = down_source.shape[2]
    both = parts * sources
    blocks = next(b for b in (4, 2, 1) if own % (b * 128) == 0)
    width = own // blocks
    vmem = pl.BlockSpec(memory_space=pltpu.VMEM)
    dma = pltpu.SemaphoreType.DMA
    result = pl.pallas_call(
        functools.partial(sweeps, layers, peers, blocks),
        out_shape=jax.ShapeDtypeStruct((both, own), F32),
        in_specs=[pl.BlockSpec(memory_space=pl.ANY), vmem, vmem],
        out_specs=vmem,
        scratch_shapes=[
            pltpu.VMEM((parts, own, wide), BF16),
            pltpu.VMEM((blocks, peers, both, width), BF16),
            pltpu.VMEM((blocks, both, width), BF16),
            pltpu.VMEM((peers, blocks, both, width), BF16),
            pltpu.VMEM((peers, blocks, both, width), BF16),
            pltpu.VMEM((blocks, both, width), BF16),
            pltpu.VMEM((blocks, both, width), BF16),
            pltpu.VMEM((both, own), F32),
            pltpu.VMEM((peers, both, own), F32),
            dma((blocks, 2)),
            dma((blocks,)), dma((blocks,)),
            dma((blocks, peers)), dma((blocks, peers)),
            dma((blocks,)), dma((blocks,)),
            dma((peers, blocks)), dma((peers, blocks)),
        ],
        compiler_params=pltpu.CompilerParams(
            collective_id=0, has_side_effects=True, vmem_limit_bytes=60 * 1024 * 1024),
    )(green[0], down_source.reshape(both, own), up_source.reshape(both, own))
    return result.reshape(1, parts, sources, own)


def solution(mesh):
    in_specs = (
        P("sweep", None, "layer", None),
        P("sweep", None, None, "layer"),
        P("sweep", None, None, "layer"),
    )
    out_specs = P("sweep", None, None, "layer")
    body = functools.partial(local, mesh.shape["sweep"], mesh.shape["layer"])
    return jax.shard_map(body, mesh=mesh, in_specs=in_specs, out_specs=out_specs, check_vma=False)
```

```python
import functools

import jax
import jax.numpy as jnp
from jax import lax
from jax.experimental import pallas as pl
from jax.experimental.pallas import tpu as pltpu
from jax.sharding import PartitionSpec as P

MESH = pl.DeviceIdType.MESH
F32, BF16 = jnp.float32, jnp.bfloat16
BY_LANES = (((1,), (1,)), ((), ()))


def turned(trace):
    half = trace.shape[0] // 2
    return jnp.concatenate([-trace[half:], trace[:half]], axis=0)


def rows_dot(trace, block):
    return lax.dot_general(trace, block, BY_LANES, preferred_element_type=F32)


def cols_dot(trace, block):
    return jnp.dot(trace, block, preferred_element_type=F32)


def sweeps(layers, peers, blocks, green, down_src, up_src, total,
           matrix, gathered, incoming, part_out, part_in, out_down, out_up, base, acc,
           load_sem, dsend, drecv, gsend, grecv, usend, urecv, psend, precv):
    z, j = lax.axis_index("sweep"), lax.axis_index("layer")
    own = down_src.shape[1]
    width = own // blocks
    odd = lax.rem(z, 2) == 1

    def span(k):
        return pl.ds(pl.multiple_of(k * width, width), width)

    def cols(i, k):
        return pl.ds(pl.multiple_of(i * own + k * width, width), width)

    def peer(d):
        return lax.rem(j + d, peers)

    def load(m, part):
        return pltpu.make_async_copy(
            green.at[part, span(m)], matrix.at[part, span(m)], load_sem.at[m, part])

    def wait_load(m):
        load(m, 0).wait()
        load(m, 1).wait()

    def remote(src, dst, send, recv, to):
        return pltpu.make_async_remote_copy(
            src_ref=src, dst_ref=dst, send_sem=send, recv_sem=recv, device_id=to, device_id_type=MESH)

    def pass_down(k):
        return remote(out_down.at[k], gathered.at[k, j], dsend.at[k], drecv.at[k], {"sweep": z + 1})

    def pass_up(k):
        return remote(out_up.at[k], incoming.at[k], usend.at[k], urecv.at[k], {"sweep": z - 1})

    def relay(k, d):
        return remote(gathered.at[k, j], gathered.at[k, j], gsend.at[k, d], grecv.at[k, j], {"layer": peer(d)})

    def relayed(k, d):
        i = peer(d)
        return remote(gathered.at[k, i], gathered.at[k, i], gsend.at[k, d], grecv.at[k, i], {"layer": i})

    def share(d, k):
        i = peer(d)
        return remote(part_out.at[i, k], part_in.at[j, k], psend.at[d, k], precv.at[j, k], {"layer": i})

    def shared(d, k):
        i = peer(d)
        return remote(part_out.at[i, k], part_in.at[i, k], psend.at[d, k], precv.at[i, k], {"layer": i})

    def share_all(d):
        i = peer(d)
        return remote(part_out.at[i], part_in.at[j], psend.at[d, 0], precv.at[j, 0], {"layer": i})

    def shared_all(d):
        i = peer(d)
        return remote(part_out.at[i], part_in.at[i], psend.at[d, 0], precv.at[i, 0], {"layer": i})

    for m in range(blocks):
        load(m, 0).start()
        load(m, 1).start()

    barrier = pltpu.get_barrier_semaphore()
    for d in range(1, peers):
        pl.semaphore_signal(barrier, inc=1, device_id={"layer": peer(d)}, device_id_type=MESH)
    for step in (1, layers - 1):
        pl.semaphore_signal(barrier, inc=1, device_id={"sweep": lax.rem(z + step, layers)}, device_id_type=MESH)
    pl.semaphore_wait(barrier, peers + 1)

    def finish_down(k, value):
        sum_of = up_src[:, span(k)] + value

        @pl.when(z < layers - 1)
        def _():
            base[:, span(k)] = sum_of
            out_down[k] = value.astype(BF16)
            pass_down(k).start()

        @pl.when(z == layers - 1)
        def _():
            total[:, span(k)] = sum_of
            out_up[k] = sum_of.astype(BF16)
            pass_up(k).start()

    def take(k):
        relayed_own = remote(
            out_down.at[k], gathered.at[k, j], dsend.at[k], drecv.at[k], {"sweep": z})
        relayed_own.wait_recv()
        for d in range(1, peers):
            relay(k, d).start()

    def wait_gather(k):
        for d in range(1, peers):
            relayed(k, d).wait_recv()

    def wait_up(k):
        remote(out_up.at[k], incoming.at[k], usend.at[k], urecv.at[k], {"sweep": z}).wait_recv()

    def down_term(m, ks):
        value = None
        for k in ks:
            for i in range(peers):
                trace = gathered[k, i]
                term = rows_dot(trace, matrix[0, span(m), cols(i, k)])
                value = term if value is None else value + term
                value = value + rows_dot(turned(trace), matrix[1, span(m), cols(i, k)])
        return value

    @pl.when(z == 0)
    def _():
        @pl.loop(0, blocks)
        def _(k):
            finish_down(k, down_src[:, span(k)])

        @pl.loop(0, blocks)
        def _(m):
            wait_load(m)

    @pl.when(z == 1)
    def _():
        @pl.loop(0, blocks)
        def _(k):
            take(k)

        @pl.loop(0, blocks)
        def _(k):
            wait_gather(k)

        @pl.loop(0, blocks)
        def _(m):
            wait_load(m)
            finish_down(m, down_src[:, span(m)] + down_term(m, range(blocks)))

    @pl.when(odd & (z > 1))
    def _():
        early = blocks // 2

        @pl.loop(0, blocks)
        def _(m):
            wait_load(m)

        base[...] = down_src[...]

        @pl.loop(0, blocks)
        def _(k):
            take(k)

        @pl.loop(0, early)
        def _(k):
            wait_gather(k)
            for m in range(blocks):
                base[:, span(m)] += down_term(m, [k])

        @pl.loop(early, blocks)
        def _(k):
            wait_gather(k)

        @pl.loop(0, blocks)
        def _(m):
            finish_down(m, base[:, span(m)] + down_term(m, range(early, blocks)))

    @pl.when(jnp.logical_not(odd) & (z > 0))
    def _():
        @pl.loop(0, blocks)
        def _(m):
            wait_load(m)

        base[...] = down_src[...]
        take(0)

        @pl.loop(0, blocks - 1)
        def _(k):
            take(k + 1)
            wait_gather(k)
            for m in range(blocks):
                base[:, span(m)] += down_term(m, [k])

        wait_gather(blocks - 1)
        for m in range(blocks):
            finish_down(m, base[:, span(m)] + down_term(m, [blocks - 1]))

    def finish_up(k):
        value = acc[j, :, span(k)]
        for d in range(1, peers):
            value = value + part_in[peer(d), k].astype(F32)
        value = base[:, span(k)] + value
        total[:, span(k)] = value

        @pl.when(z > 0)
        def _():
            out_up[k] = value.astype(BF16)
            pass_up(k).start()

    @pl.when(odd & (z < layers - 1))
    def _():
        @pl.loop(0, blocks)
        def _(k):
            wait_up(k)

        def reduce(k):
            for d in range(1, peers):
                shared(d, k).wait_recv()
            finish_up(k)

        @pl.loop(0, blocks)
        def _(k):
            for d in list(range(1, peers)) + [0]:
                i = peer(d)
                value = None
                for r in range(blocks):
                    trace = incoming[r]
                    term = cols_dot(trace, matrix[0, span(r), cols(i, k)])
                    value = term if value is None else value + term
                    value = value + cols_dot(turned(trace), matrix[1, span(r), cols(i, k)])
                if d:
                    part_out[i, k] = value.astype(BF16)
                else:
                    acc[i, :, span(k)] = value
            for d in range(1, peers):
                share(d, k).start()

            @pl.when(k > 0)
            def _():
                reduce(k - 1)

        reduce(blocks - 1)

        @pl.loop(0, blocks)
        def _(k):
            for d in range(1, peers):
                share(d, k).wait_send()

    @pl.when(jnp.logical_not(odd) & (z < layers - 1))
    def _():
        acc[...] = jnp.zeros_like(acc)

        def up_term(trace, r, i, k):
            value = cols_dot(trace, matrix[0, span(r), cols(i, k)])
            return value + cols_dot(turned(trace), matrix[1, span(r), cols(i, k)])

        @pl.loop(0, blocks - 1)
        def _(r):
            wait_up(r)
            trace = incoming[r]
            for i in range(peers):
                for k in range(blocks):
                    acc[i, :, span(k)] += up_term(trace, r, i, k)

        wait_up(blocks - 1)
        last = incoming[blocks - 1]
        for d in range(1, peers):
            i = peer(d)
            for k in range(blocks):
                value = acc[i, :, span(k)] + up_term(last, blocks - 1, i, k)
                part_out[i, k] = value.astype(BF16)
            share_all(d).start()
        for k in range(blocks):
            acc[j, :, span(k)] += up_term(last, blocks - 1, j, k)
        for d in range(1, peers):
            shared_all(d).wait_recv()

        @pl.loop(0, blocks)
        def _(k):
            finish_up(k)

        for d in range(1, peers):
            share_all(d).wait_send()

    @pl.when(z < layers - 1)
    def _():
        @pl.loop(0, blocks)
        def _(k):
            pass_down(k).wait_send()

    @pl.when(z > 0)
    def _():
        @pl.loop(0, blocks)
        def _(k):
            pass_up(k).wait_send()
            for d in range(1, peers):
                relay(k, d).wait_send()


def local(layers, peers, green, down_source, up_source):
    _one, parts, own, wide = green.shape
    sources = down_source.shape[2]
    both = parts * sources
    blocks = next(b for b in (4, 2, 1) if own % (b * 128) == 0)
    width = own // blocks
    vmem = pl.BlockSpec(memory_space=pltpu.VMEM)
    dma = pltpu.SemaphoreType.DMA
    result = pl.pallas_call(
        functools.partial(sweeps, layers, peers, blocks),
        out_shape=jax.ShapeDtypeStruct((both, own), F32),
        in_specs=[pl.BlockSpec(memory_space=pl.ANY), vmem, vmem],
        out_specs=vmem,
        scratch_shapes=[
            pltpu.VMEM((parts, own, wide), BF16),
            pltpu.VMEM((blocks, peers, both, width), BF16),
            pltpu.VMEM((blocks, both, width), BF16),
            pltpu.VMEM((peers, blocks, both, width), BF16),
            pltpu.VMEM((peers, blocks, both, width), BF16),
            pltpu.VMEM((blocks, both, width), BF16),
            pltpu.VMEM((blocks, both, width), BF16),
            pltpu.VMEM((both, own), F32),
            pltpu.VMEM((peers, both, own), F32),
            dma((blocks, 2)),
            dma((blocks,)), dma((blocks,)),
            dma((blocks, peers)), dma((blocks, peers)),
            dma((blocks,)), dma((blocks,)),
            dma((peers, blocks)), dma((peers, blocks)),
        ],
        compiler_params=pltpu.CompilerParams(
            collective_id=0, has_side_effects=True, vmem_limit_bytes=60 * 1024 * 1024),
    )(green[0], down_source.reshape(both, own), up_source.reshape(both, own))
    return result.reshape(1, parts, sources, own)


def solution(mesh):
    in_specs = (
        P("sweep", None, "layer", None),
        P("sweep", None, None, "layer"),
        P("sweep", None, None, "layer"),
    )
    out_specs = P("sweep", None, None, "layer")
    body = functools.partial(local, mesh.shape["sweep"], mesh.shape["layer"])
    return jax.shard_map(body, mesh=mesh, in_specs=in_specs, out_specs=out_specs, check_vma=False)
```
